512 devices in a mesh: sub: 128 (over z, y, core), leaf: 4 (over x).
Axes of the slice: x: 4, y: 8, z: 8, core: 2. Of those that a mesh axis runs over, the one named last changes fastest.
Arguments:
- child_row: int32 [256], P('sub'), may hold values from 0 to 255, each once
- counts: int32 [256], P('sub'), may hold values from 1 to 16, as said below
- live_mask: int32 [256, 16, 1326], P('sub', 'leaf'), may hold values 0 or 1
- hand_rank: int32 [256, 16, 1326], P('sub', 'leaf'), may hold values from 0 to 7461
- bet_size: float32 [256, 8], P('sub'), may hold values from 0.25 to 4
- pot_size: float32 [256], P('sub'), may hold values from 4 to 16
- trunk_ranges: float32 [256, 2, 1326], P('sub'), may hold values from 0.05 to 1
- trunk_values: float32 [256, 1326], P('sub'), may hold values from -8 to 8
Outputs:
- root_values: float32 [256, 2, 1326], P('sub')
The draws below stay inside these ranges and needn't reach their ends.
Inputs may be any that keep to these rules, and one draw needn't show every extreme that they name: Subgame s reads and returns row child_row[s] of the trunk's arrays; every row is named by exactly one subgame. Leaf blocks b < counts[s] of subgame s are used; some subgame uses all 16.
All inputs are finite; a program needn't handle non-finite values. No bound on the sum of `live_mask` on one device may be relied on, other than what follows from the above.
Results may differ from the reference program's by a relative error of at most 0.0004.
Values sent between devices are 32-bit elements; how exact they have to be, the bound alone decides.
No kernel may reach another device: no remote copies, remote signals or barrier semaphores. Data moves between devices by JAX's collectives and lax.ppermute only.
A program may use at most 64 MiB of HBM per device.

```python
import math
import jax
import jax.numpy as jnp
from jax import lax

H = 1326
ACT = 8
ITERS = 4
S = 256
MAXB = 16


def draw_counts(key, part):
    key_one, key_two, key_three = jax.random.split(key, 3)
    first_draw = jax.random.randint(key_one, (S,), 1, MAXB + 1)
    second_draw = jax.random.randint(key_two, (S,), 1, MAXB + 1)
    picked = jnp.minimum(first_draw, second_draw)
    forced_at = jax.random.randint(key_three, (), 0, S)
    return jnp.where(jnp.arange(S) == forced_at, MAXB, picked).astype(jnp.int32)


def set_ends(array, key, smallest, high):
    extent = array.shape
    spot = [jax.random.randint(jax.random.fold_in(key, axis), (), 0, extent[axis]) for axis in range(len(extent))]
    array = array.at[tuple(spot)].set(smallest)
    longest = extent.index(max(extent))
    spot[longest] = (spot[longest] + 1) % extent[longest]
    return array.at[tuple(spot)].set(high)


def level_of(stream_key, extent, shards, low, high):
    factor_of = 1.0
    for dim, blocks in shards:
        heights = jax.random.uniform(jax.random.fold_in(jax.random.fold_in(stream_key, 6), dim), (blocks,), jnp.float32, low / len(shards), high / len(shards))
        factor_of = factor_of * jnp.repeat(jnp.exp(heights), extent[dim] // blocks).reshape((-1,) + (1,) * (len(extent) - 1 - dim))
    return factor_of


def normal_values(key, extent, width, limit, cuts=(), dtype=jnp.bfloat16):
    factor_of = level_of(key, extent, cuts, -0.22, 0.18) if cuts else 1.0
    result = jax.random.normal(key, extent, jnp.float32) * width * factor_of
    return jnp.minimum(jnp.maximum(result, -limit), limit).astype(dtype)


def setup_inputs(seed: int = 0) -> dict:
    key_list = jax.random.split(jax.random.key(seed), 9)
    child_row = jax.random.permutation(key_list[0], S).astype(jnp.int32)
    counts = draw_counts(jax.random.fold_in(key_list[8], 71), 0)
    live_mask = set_ends((jax.random.randint(key_list[2], (S, MAXB, H), 0, 8) < 7).astype(jnp.int32), jax.random.fold_in(key_list[2], 1), 0, 1)
    hand_rank = set_ends(jax.random.randint(key_list[3], (S, MAXB, H), 0, 7462), jax.random.fold_in(key_list[3], 1), 0, 7461).astype(jnp.int32)
    bet_size = jnp.clip(jnp.exp(math.log(4.0) - 2.7725887 * jax.random.uniform(key_list[4], (S, ACT), jnp.float32) ** level_of(key_list[4], (S, ACT), ((0, 128),), -0.2, 0.2)), 0.25, 4.0)
    pot_size = jnp.clip(jnp.exp(math.log(16.0) - 1.3862944 * jax.random.uniform(key_list[5], (S,), jnp.float32) ** level_of(key_list[5], (S,), ((0, 128),), -0.2, 0.2)), 4.0, 16.0)
    trunk_ranges = jnp.clip(jnp.exp(math.log(1.0) - 2.9957323 * jax.random.uniform(key_list[6], (S, 2, H), jnp.float32) ** level_of(key_list[6], (S, 2, H), ((0, 128),), -0.2, 0.2)), 0.05, 1.0)
    trunk_values = normal_values(key_list[7], (S, H), 1.5, 8.0, ((0, 128),), jnp.float32)
    return {"child_row": child_row, "counts": counts, "live_mask": live_mask, "hand_rank": hand_rank, "bet_size": bet_size, "pot_size": pot_size, "trunk_ranges": trunk_ranges, "trunk_values": trunk_values}


smooth = 0.1


def regret_match(positive, total_sum, option_count):
    return (positive + smooth) / (total_sum + option_count * smooth)


def solve_one(packed):
    used_count, live_slab, rank_slab, bet_row, pot_value, ranges, values = packed
    live_real = live_slab.astype(jnp.float32)
    block_ids = jnp.arange(MAXB)
    block_weight = jnp.where(block_ids < used_count, 1.0, 0.0).astype(jnp.float32) / used_count.astype(jnp.float32)
    sign_table = jnp.sign(rank_slab[:, :, None] - rank_slab[:, None, :]).astype(jnp.float32)
    showdown = sign_table * live_real[:, :, None] * live_real[:, None, :]
    own_range = ranges[0]
    opp_range = ranges[1]
    factor = pot_value * (1.0 + bet_row) / H
    regret_own = jnp.zeros((ACT, H), jnp.float32)
    call_regret = jnp.zeros((MAXB, ACT, H), jnp.float32)
    fold_regret = jnp.zeros((MAXB, ACT, H), jnp.float32)
    follow_regret = jnp.zeros((H,), jnp.float32)
    stop_regret = jnp.zeros((H,), jnp.float32)
    for step_index in range(ITERS):
        own_strategy = regret_match(regret_own, jnp.sum(regret_own, axis=0), ACT)
        call_prob = regret_match(call_regret, call_regret + fold_regret, 2)
        follow = regret_match(follow_regret, follow_regret + stop_regret, 2)
        reach_own = (own_range[None, :] * own_strategy).astype(jnp.bfloat16)
        entering = opp_range * follow
        reach_call = (entering[None, None, :] * call_prob).astype(jnp.bfloat16)
        reach_fold = entering[None, None, :] * (1.0 - call_prob)
        own_real = reach_own.astype(jnp.float32)
        columns = jnp.concatenate([reach_call.astype(jnp.float32), jnp.broadcast_to(own_real[None], (MAXB, ACT, H))], axis=1)
        applied = jnp.einsum('bij,bkj->bki', showdown, columns, precision=lax.Precision.HIGHEST)
        showdown_own = applied[:, :ACT]
        showdown_opp = applied[:, ACT:]
        fold_mass = jnp.sum(live_real[:, None, :] * reach_fold, axis=-1) / H
        own_mass = jnp.sum(live_real[:, None, :] * own_real[None], axis=-1) / H
        per_block = factor[None, :, None] * showdown_own + live_real[:, None, :] * (pot_value * fold_mass)[:, :, None]
        value_own = jnp.sum(block_weight[:, None, None] * per_block, axis=0)
        call_value = factor[None, :, None] * showdown_opp
        fold_value = -live_real[:, None, :] * (pot_value * own_mass)[:, :, None]
        node_value = call_prob * call_value + (1.0 - call_prob) * fold_value
        follow_value = jnp.sum(block_weight[:, None, None] * node_value, axis=(0, 1))
        gadget_value = follow * follow_value + (1.0 - follow) * values
        root_value = jnp.sum(own_strategy * value_own, axis=0)
        if step_index + 1 < ITERS:
            regret_own = jnp.maximum(regret_own + value_own - root_value[None, :], 0.0)
            call_regret = jnp.maximum(call_regret + call_value - node_value, 0.0)
            fold_regret = jnp.maximum(fold_regret + fold_value - node_value, 0.0)
            follow_regret = jnp.maximum(follow_regret + follow_value - gadget_value, 0.0)
            stop_regret = jnp.maximum(stop_regret + values - gadget_value, 0.0)
    return jnp.stack([root_value, jnp.maximum(values, follow_value)], axis=0)


def reference(child_row, counts, live_mask, hand_rank, bet_size, pot_size, trunk_ranges, trunk_values):
    gathered_ranges = trunk_ranges[child_row]
    gathered_values = trunk_values[child_row]
    results = lax.map(solve_one, (counts, live_mask, hand_rank, bet_size, pot_size, gathered_ranges, gathered_values))
    return jnp.zeros((S, 2, H), jnp.float32).at[child_row].set(results)
```

```python
import jax
import jax.numpy as jnp
from jax import lax
from jax.experimental import pallas as pl
from jax.experimental.pallas import tpu as pltpu
from jax.sharding import Mesh
from jax.sharding import PartitionSpec as P

ACT = 8
ITERS = 4
BLOCKS = 16
SUB = ("z", "y", "c")
NZ, NY, NC, NX = 8, 8, 2, 4
LANES = 128
smooth = 0.1
F32 = jnp.float32
BF16 = jnp.bfloat16
F8 = jnp.float8_e4m3fn
SMEM = pl.BlockSpec(memory_space=pltpu.SMEM)
VMEM = pl.BlockSpec(memory_space=pltpu.VMEM)


def round_up(value, unit):
    return -(-value // unit) * unit


def row_parts(row):
    slot = lax.rem(row, 2)
    core = lax.rem(lax.div(row, 2), NC)
    y = lax.rem(lax.div(row, 2 * NC), NY)
    z = lax.div(row, 2 * NC * NY)
    return z, y, core, slot


def pack_rows(ids_ref, ranges_ref, values_ref, out_ref, rows_ref):
    hands = values_ref.shape[-1]
    full = hands // LANES
    rest = hands - full * LANES
    x = ids_ref[3]
    rows_ref[...] = jnp.zeros(rows_ref.shape, F32)
    for s in range(2):
        sources = (ranges_ref[s, 0:1, :], ranges_ref[s, 1:2, :], values_ref[s : s + 1, :])
        for v, line in enumerate(sources):
            for r in range(full):
                at = v * full + r
                rows_ref[s, at : at + 1, :] = line[:, r * LANES : (r + 1) * LANES]
            tail_row = 3 * full + v // 2
            tail_lane = (v % 2) * (LANES // 2)
            rows_ref[s, tail_row : tail_row + 1, tail_lane : tail_lane + rest] = line[:, full * LANES :]
    for s in range(2):
        piece = rows_ref[s, pl.ds(pl.multiple_of(8 * x, 8), 8), :]
        for d in range(out_ref.shape[0]):
            out_ref[d, s] = piece


def select_rows(wants_ref, arrived_ref, out_ref):
    for y in range(NY):
        for k in range(2):
            z, _, core, slot = row_parts(wants_ref[y, k])
            piece = arrived_ref[z * NC + core, slot]
            for x in (2 * k, 2 * k + 1):
                out_ref[y, x] = piece


def solve_kernel(
    ids_ref, child_ref, counts_ref, bet_ref, pot_ref, blocks_ref, rows_ref, out_ref,
    rank_ref, live_ref, sign_ref, column_ref, vec_ref, lhs_ref, prob_ref, call_ref, fold_ref, pack_ref,
):
    hands = blocks_ref.shape[-1]
    full = hands // LANES
    rest = hands - full * LANES
    width = rank_ref.shape[-1]
    deep = lhs_ref.shape[-1]
    core = ids_ref[2]
    x = ids_ref[3]
    k = lax.div(x, 2)
    active = lax.rem(x, 2) == core
    count = jnp.where(active, counts_ref[k], 0)
    pot = pot_ref[k]

    rank_ref[...] = jnp.zeros(rank_ref.shape, F32)
    live_ref[...] = jnp.zeros(live_ref.shape, F32)
    for source in range(NX):
        rank_ref[4 * source : 4 * source + 4, 0:hands] = blocks_ref[source, 0].astype(F32)
        live_ref[4 * source : 4 * source + 4, 0:hands] = blocks_ref[source, 1].astype(F32)

    for t in range(width // LANES):
        column_ref[t * LANES : (t + 1) * LANES, :] = rank_ref[:, t * LANES : (t + 1) * LANES].T
    tall = round_up(hands, 32)
    for b in range(BLOCKS):

        @pl.when(b < count)
        def _():
            line = rank_ref[b : b + 1, :]

            def chunk(q, carry):
                at = pl.multiple_of(q * 32, 32)
                column = column_ref[pl.ds(at, 32), b : b + 1]
                signs = jnp.clip(line - column, -1.0, 1.0)
                sign_ref[b, pl.ds(at, 32), 0:width] = signs.astype(F8)
                return carry

            lax.fori_loop(0, tall // 32, chunk, 0, unroll=2)
            sign_ref[b, tall:deep, :] = jnp.zeros((deep - tall, deep), F8)

    _, y, _, _ = row_parts(child_ref[k])
    vec_ref[...] = jnp.zeros(vec_ref.shape, F32)
    for v in range(3):
        for r in range(full):
            at = v * full + r
            vec_ref[v : v + 1, r * LANES : (r + 1) * LANES] = rows_ref[y, at // 8, at % 8 : at % 8 + 1, :]
        at = 3 * full + v // 2
        tail = rows_ref[y, at // 8, at % 8 : at % 8 + 1, :]
        if v % 2:
            tail = pltpu.roll(tail, LANES // 2, 1)
        vec_ref[v : v + 1, full * LANES : hands] = tail[:, 0:rest]
    own_range = vec_ref[0:1, :]
    opp_range = vec_ref[1:2, :]
    values = vec_ref[2:3, :]

    lane_rows = lax.broadcasted_iota(jnp.int32, (ACT, 1), 0)
    bets = jnp.zeros((ACT, 1), F32)
    for a in range(ACT):
        bets = jnp.where(lane_rows == a, bet_ref[k, a], bets)
    factor = pot * (1.0 + bets) / hands
    weight = 1.0 / jnp.broadcast_to(count.astype(F32), (1, 1))
    lhs_ref[:, width:deep] = jnp.zeros((2 * ACT, deep - width), BF16)

    regret_own = jnp.zeros((ACT, width), F32)
    follow_regret = jnp.zeros((1, width), F32)
    stop_regret = jnp.zeros((1, width), F32)
    for step in range(ITERS):
        first = step == 0
        last = step + 1 == ITERS
        strategy = (regret_own + smooth) / (jnp.sum(regret_own, axis=0, keepdims=True) + ACT * smooth)
        follow = (follow_regret + smooth) / (follow_regret + stop_regret + 2 * smooth)
        entering = opp_range * follow
        reach_own = (own_range * strategy).astype(BF16).astype(F32)

        def block(b, carry):
            value_sum, node_sum = carry
            live = live_ref[pl.ds(b, 1), :]
            prob = jnp.full((ACT, width), 0.5, F32) if first else prob_ref[b]
            live_own = reach_own * live
            lhs_ref[0:ACT, 0:width] = (entering * prob).astype(BF16) * live.astype(BF16)
            lhs_ref[ACT : 2 * ACT, 0:width] = live_own.astype(BF16)
            fold_mass = jnp.sum(live * (entering * (1.0 - prob)), axis=1, keepdims=True) / hands
            own_mass = jnp.sum(live_own, axis=1, keepdims=True) / hands

            def multiply(*sums):
                for n in range(deep // 256):
                    for j in range(deep // 256):
                        tile = sign_ref[b, 256 * j : 256 * (j + 1), 256 * n : 256 * (n + 1)]
                        pltpu.matmul_push_rhs(tile, staging_register=j % 2, mxu_index=n % 2)
                        pltpu.matmul_acc_lhs(sums[n], lhs_ref[:, 256 * j : 256 * (j + 1)], load_staged_rhs=j % 2)
                return jnp.concatenate([pltpu.matmul_pop(s) for s in sums], axis=1)[:, :width]

            applied = pl.run_scoped(
                multiply, *[pltpu.ACC(n % 2)((2 * ACT, 256), F32) for n in range(deep // 256)]
            )
            showdown_own = applied[0:ACT] * live
            showdown_opp = applied[ACT : 2 * ACT] * live
            value_sum = value_sum + weight * (factor * showdown_own + live * (pot * fold_mass))
            call_value = factor * showdown_opp
            fold_value = -live * (pot * own_mass)
            node_value = prob * call_value + (1.0 - prob) * fold_value
            node_sum = node_sum + weight * node_value
            if not last:
                call = call_value - node_value
                fold = fold_value - node_value
                if not first:
                    call = call_ref[b] + call
                    fold = fold_ref[b] + fold
                call = jnp.maximum(call, 0.0)
                fold = jnp.maximum(fold, 0.0)
                call_ref[b] = call
                fold_ref[b] = fold
                prob_ref[b] = (call + smooth) / (call + fold + 2 * smooth)
            return value_sum, node_sum

        zeros = jnp.zeros((ACT, width), F32)
        value_own, node_sum = lax.fori_loop(0, count, block, (zeros, zeros))
        follow_value = jnp.sum(node_sum, axis=0, keepdims=True)
        gadget_value = follow * follow_value + (1.0 - follow) * values
        root_value = jnp.sum(strategy * value_own, axis=0, keepdims=True)
        if not last:
            regret_own = jnp.maximum(regret_own + value_own - root_value, 0.0)
            follow_regret = jnp.maximum(follow_regret + follow_value - gadget_value, 0.0)
            stop_regret = jnp.maximum(stop_regret + values - gadget_value, 0.0)

    pack_ref[...] = jnp.zeros(pack_ref.shape, F32)
    for v, line in enumerate((root_value, jnp.maximum(values, follow_value))):
        for r in range(full):
            at = v * full + r
            pack_ref[at // 6, at % 6 : at % 6 + 1, :] = line[:, r * LANES : (r + 1) * LANES]
        at = 2 * full
        lane = v * (LANES // 2)
        pack_ref[at // 6, at % 6 : at % 6 + 1, lane : lane + rest] = line[:, full * LANES : hands]
    for y in range(NY):
        out_ref[y] = pack_ref[...]


def route_results(ids_ref, wants_ref, arrived_ref, out_ref):
    here = ids_ref[1]
    core_here = ids_ref[2]
    out_ref[...] = jnp.zeros(out_ref.shape, F32)
    for y in range(NY):
        for k in range(2):
            z, row_y, core, slot = row_parts(wants_ref[y, k])

            @pl.when(row_y == here)
            def _():
                piece = arrived_ref[y, 2 * k + core_here]
                for x in range(NX):
                    out_ref[(z * NC + core) * NX + x, slot] = piece


def unpack_results(arrived_ref, out_ref):
    hands = out_ref.shape[-1]
    full = hands // LANES
    rest = hands - full * LANES
    for s in range(2):
        lines = []
        for x in range(NX):
            total = arrived_ref[x, s]
            for source in range(1, NZ * NC):
                total = total + arrived_ref[source * NX + x, s]
            lines.append(total)
        for v in range(2):
            for r in range(full):
                at = v * full + r
                out_ref[s, v : v + 1, r * LANES : (r + 1) * LANES] = lines[at // 6][at % 6 : at % 6 + 1, :]
            at = 2 * full
            tail = lines[at // 6][at % 6 : at % 6 + 1, :]
            if v:
                tail = pltpu.roll(tail, LANES // 2, 1)
            out_ref[s, v : v + 1, full * LANES : hands] = tail[:, 0:rest]


def exchange(parts, axes):
    return lax.all_to_all(parts, axes, split_axis=0, concat_axis=0, tiled=True)


def shards(child_row, counts, live_mask, hand_rank, bet_size, pot_size, trunk_ranges, trunk_values):
    hands = trunk_ranges.shape[-1]
    width = round_up(hands, LANES)
    deep = round_up(hands, 256)
    ids = jnp.stack([lax.axis_index(a) for a in ("z", "y", "c", "leaf")])

    packed = pl.pallas_call(
        pack_rows,
        out_shape=jax.ShapeDtypeStruct((NZ * NC, 2, 8, LANES), F32),
        in_specs=[SMEM, VMEM, VMEM],
        out_specs=VMEM,
        scratch_shapes=[pltpu.VMEM((2, 32, LANES), F32)],
        name="pack_rows",
    )(ids, trunk_ranges, trunk_values)
    gathered = exchange(packed, ("z", "c"))
    wants = exchange(jnp.broadcast_to(child_row, (NY, 2)), "y")
    both = jnp.stack([hand_rank, live_mask], axis=1)
    blocks = exchange(jnp.repeat(both, 2, axis=0), "leaf")
    selected = pl.pallas_call(
        select_rows,
        out_shape=jax.ShapeDtypeStruct((NY, NX, 8, LANES), F32),
        in_specs=[SMEM, VMEM],
        out_specs=VMEM,
        name="select_rows",
    )(wants, gathered)
    rows = exchange(selected.reshape(NY * NX, 8, LANES), ("y", "leaf")).reshape(NY, NX, 8, LANES)
    results = pl.pallas_call(
        solve_kernel,
        out_shape=jax.ShapeDtypeStruct((NY, NX, 8, LANES), F32),
        in_specs=[SMEM, SMEM, SMEM, SMEM, SMEM, VMEM, VMEM],
        out_specs=VMEM,
        scratch_shapes=[
            pltpu.VMEM((BLOCKS, width), F32),
            pltpu.VMEM((BLOCKS, width), F32),
            pltpu.VMEM((BLOCKS, deep, deep), F8),
            pltpu.VMEM((width, BLOCKS), F32),
            pltpu.VMEM((8, width), F32),
            pltpu.VMEM((2 * ACT, deep), BF16),
            pltpu.VMEM((BLOCKS, ACT, width), F32),
            pltpu.VMEM((BLOCKS, ACT, width), F32),
            pltpu.VMEM((BLOCKS, ACT, width), F32),
            pltpu.VMEM((NX, 8, LANES), F32),
        ],
        compiler_params=pltpu.CompilerParams(vmem_limit_bytes=56 * 1024 * 1024),
        name="solve",
    )(ids, child_row, counts, bet_size, pot_size, blocks, rows)
    back = exchange(results.reshape(NY * NX, 8, LANES), ("y", "leaf")).reshape(NY, NX, 8, LANES)
    routed = pl.pallas_call(
        route_results,
        out_shape=jax.ShapeDtypeStruct((NZ * NC * NX, 2, 8, LANES), F32),
        in_specs=[SMEM, SMEM, VMEM],
        out_specs=VMEM,
        name="route_results",
    )(ids, wants, back)
    home = exchange(routed, ("z", "c", "leaf"))
    return pl.pallas_call(
        unpack_results,
        out_shape=jax.ShapeDtypeStruct(trunk_ranges.shape, F32),
        in_specs=[VMEM],
        out_specs=VMEM,
        name="unpack_results",
    )(home)


def solution(mesh):
    split = Mesh(mesh.devices.reshape(NZ, NY, NC, NX), ("z", "y", "c", "leaf"))
    in_specs = (
        P(SUB),
        P(SUB),
        P(SUB, "leaf", None),
        P(SUB, "leaf", None),
        P(SUB, None),
        P(SUB),
        P(SUB, None, None),
        P(SUB, None),
    )
    return jax.shard_map(
        shards, mesh=split, in_specs=in_specs, out_specs=P(SUB, None, None), check_vma=False
    )
```
